32 devices in a mesh: dp: 1 (over z), cp: 4 (over y), tp: 8 (over x, core).
Axes of the slice: x: 4, y: 4, z: 1, core: 2. Of those that a mesh axis runs over, the one named last changes fastest.
The devices are a block of a 4x4x8 slice.
Arguments:
- x: bfloat16 [1, 8192, 5120], P('dp', ('cp', 'tp'))
- g_attn: bfloat16 [5120], replicated
- w_q: bfloat16 [5120, 40, 128], P(None, 'tp')
- w_k: bfloat16 [5120, 8, 128], P(None, 'tp')
- w_v: bfloat16 [5120, 8, 128], P(None, 'tp')
- w_o: bfloat16 [40, 128, 5120], P('tp')
- g_mlp: bfloat16 [5120], replicated
- w_gate: bfloat16 [5120, 27648], P(None, 'tp')
- w_up: bfloat16 [5120, 27648], P(None, 'tp')
- w_down: bfloat16 [27648, 5120], P('tp')
Outputs:
- output: bfloat16 [1, 8192, 5120], P('dp', ('cp', 'tp'))
All inputs are finite; a program needn't handle non-finite values.
Results may differ from the reference program's by a relative error of at most 0.02.
Values are sent between devices in bfloat16 or wider.
A program may use at most 768 MiB of HBM per device.

```python
import math
import jax
import jax.numpy as jnp
from jax import lax

SEQ_LEN = 8192
MODEL_DIM = 5120
N_HEADS = 40
N_KV_HEADS = 8
HEAD_DIM = 128
FFN_DIM = 27648
CP_SIZE = 4
Q_BLOCK = 128
NORM_EPS = 1e-5
ROPE_THETA = 500000.0


def stored_positions(row_ids):
    piece_len = SEQ_LEN // (2 * CP_SIZE)
    owner_cp = row_ids // (2 * piece_len)
    within = row_ids % (2 * piece_len)
    return jnp.where(within < piece_len, owner_cp * piece_len + within,
                     (2 * CP_SIZE - 1 - owner_cp) * piece_len + within - piece_len)


def rms_norm(rows_in, gain_vec):
    rows_f32 = rows_in.astype(jnp.float32)
    mean_sq = jnp.mean(rows_f32 * rows_f32, axis=-1, keepdims=True)
    return (rows_f32 * lax.rsqrt(mean_sq + NORM_EPS) * gain_vec.astype(jnp.float32)).astype(jnp.bfloat16)


def apply_rope(heads_in, positions):
    half_dim = HEAD_DIM // 2
    inv_freq = ROPE_THETA ** (-2.0 * jnp.arange(half_dim, dtype=jnp.float32) / HEAD_DIM)
    angles = positions.astype(jnp.float32)[:, None] * inv_freq[None, :]
    angles = jnp.concatenate([angles, angles], axis=-1)[:, None, :]
    heads_f32 = heads_in.astype(jnp.float32)
    rotated = jnp.concatenate([-heads_f32[..., half_dim:], heads_f32[..., :half_dim]], axis=-1)
    return (heads_f32 * jnp.cos(angles) + rotated * jnp.sin(angles)).astype(jnp.bfloat16)


def draw_weight(key_in, weight_shape, std_dev):
    return (std_dev * jax.random.normal(key_in, weight_shape, jnp.float32)).astype(jnp.bfloat16)


def setup_inputs(seed: int = 0, part: int = 0) -> dict:
    key_list = jax.random.split(jax.random.key(seed), 10)
    qk_std = math.log(SEQ_LEN / 32.0) ** 0.25 / math.sqrt(MODEL_DIM)
    x = 0.5 * jax.random.normal(jax.random.fold_in(key_list[0], part), (1, SEQ_LEN, MODEL_DIM), jnp.float32)
    return {
        'x': x.astype(jnp.bfloat16),
        'g_attn': (0.5 + jax.random.uniform(key_list[1], (MODEL_DIM,), jnp.float32)).astype(jnp.bfloat16),
        'w_q': draw_weight(key_list[2], (MODEL_DIM, N_HEADS, HEAD_DIM), qk_std),
        'w_k': draw_weight(key_list[3], (MODEL_DIM, N_KV_HEADS, HEAD_DIM), qk_std),
        'w_v': draw_weight(key_list[4], (MODEL_DIM, N_KV_HEADS, HEAD_DIM), MODEL_DIM ** -0.5),
        'w_o': draw_weight(key_list[5], (N_HEADS, HEAD_DIM, MODEL_DIM), 2.0 * (N_HEADS * HEAD_DIM) ** -0.5),
        'g_mlp': (0.5 + jax.random.uniform(key_list[6], (MODEL_DIM,), jnp.float32)).astype(jnp.bfloat16),
        'w_gate': draw_weight(key_list[7], (MODEL_DIM, FFN_DIM), MODEL_DIM ** -0.5),
        'w_up': draw_weight(key_list[8], (MODEL_DIM, FFN_DIM), MODEL_DIM ** -0.5),
        'w_down': draw_weight(key_list[9], (FFN_DIM, MODEL_DIM), FFN_DIM ** -0.5),
    }


def reference(x, g_attn, w_q, w_k, w_v, w_o, g_mlp, w_gate, w_up, w_down):
    group_size = N_HEADS // N_KV_HEADS
    n_blocks = SEQ_LEN // Q_BLOCK
    positions = stored_positions(jnp.arange(SEQ_LEN, dtype=jnp.int32))
    x_rows = x[0]
    normed = rms_norm(x_rows, g_attn)
    q_all = jnp.dot(normed, w_q.reshape(MODEL_DIM, N_HEADS * HEAD_DIM), preferred_element_type=jnp.float32).astype(jnp.bfloat16)
    k_all = jnp.dot(normed, w_k.reshape(MODEL_DIM, N_KV_HEADS * HEAD_DIM), preferred_element_type=jnp.float32).astype(jnp.bfloat16)
    v_all = jnp.dot(normed, w_v.reshape(MODEL_DIM, N_KV_HEADS * HEAD_DIM), preferred_element_type=jnp.float32).astype(jnp.bfloat16)
    q_all = apply_rope(q_all.reshape(SEQ_LEN, N_HEADS, HEAD_DIM), positions)
    k_all = apply_rope(k_all.reshape(SEQ_LEN, N_KV_HEADS, HEAD_DIM), positions).astype(jnp.float32)
    v_all = v_all.reshape(SEQ_LEN, N_KV_HEADS, HEAD_DIM).astype(jnp.float32)
    w_o_flat = w_o.reshape(N_HEADS * HEAD_DIM, MODEL_DIM)
    score_scale = HEAD_DIM ** -0.5

    def one_block(block_in):
        q_blk, pos_blk, x_blk = block_in
        q_grp = q_blk.reshape(Q_BLOCK, N_KV_HEADS, group_size, HEAD_DIM).astype(jnp.float32)
        scores = jnp.einsum('qgrd,kgd->gqrk', q_grp, k_all) * score_scale
        visible = pos_blk[None, :, None, None] >= positions[None, None, None, :]
        scores = jnp.where(visible, scores, -1e30)
        weights = jnp.exp(scores - jnp.max(scores, axis=-1, keepdims=True))
        row_sum = jnp.sum(weights, axis=-1, keepdims=True)
        mixed_vals = jnp.einsum('gqrk,kgd->gqrd', weights.astype(jnp.bfloat16).astype(jnp.float32), v_all) / row_sum
        attn_rows = jnp.transpose(mixed_vals, (1, 0, 2, 3)).astype(jnp.bfloat16).reshape(Q_BLOCK, N_HEADS * HEAD_DIM)
        attn_proj = jnp.dot(attn_rows, w_o_flat, preferred_element_type=jnp.float32).astype(jnp.bfloat16)
        resid_rows = (x_blk.astype(jnp.float32) + attn_proj.astype(jnp.float32)).astype(jnp.bfloat16)
        normed_mlp = rms_norm(resid_rows, g_mlp)
        gate_proj = jnp.dot(normed_mlp, w_gate, preferred_element_type=jnp.float32)
        up_proj = jnp.dot(normed_mlp, w_up, preferred_element_type=jnp.float32)
        hidden = (jax.nn.silu(gate_proj) * up_proj).astype(jnp.bfloat16)
        down_proj = jnp.dot(hidden, w_down, preferred_element_type=jnp.float32).astype(jnp.bfloat16)
        return (resid_rows.astype(jnp.float32) + down_proj.astype(jnp.float32)).astype(jnp.bfloat16)

    blocks = lax.map(one_block, (q_all.reshape(n_blocks, Q_BLOCK, N_HEADS, HEAD_DIM),
                                 positions.reshape(n_blocks, Q_BLOCK),
                                 x_rows.reshape(n_blocks, Q_BLOCK, MODEL_DIM)))
    return blocks.reshape(1, SEQ_LEN, MODEL_DIM)
```

```python
import functools
import jax
import jax.numpy as jnp
from jax import lax
from jax.experimental import pallas as pl
from jax.experimental.pallas import tpu as pltpu
from jax.sharding import PartitionSpec as P

NORM_EPS = 1e-5
ROPE_THETA = 500000.0
LOG2_E = 1.4426950408889634
N_CHUNKS = 2
MLP_CHUNKS = 4


def rms_norm(rows_in, gain_vec):
    rows_f32 = rows_in.astype(jnp.float32)
    mean_sq = jnp.mean(rows_f32 * rows_f32, axis=-1, keepdims=True)
    return (rows_f32 * lax.rsqrt(mean_sq + NORM_EPS) * gain_vec.astype(jnp.float32)).astype(jnp.bfloat16)


def rope_tables(positions, head_dim):
    half_dim = head_dim // 2
    inv_freq = ROPE_THETA ** (-2.0 * jnp.arange(half_dim, dtype=jnp.float32) / head_dim)
    angles = positions.astype(jnp.float32)[:, None] * inv_freq[None, :]
    cos, sin = jnp.cos(angles), jnp.sin(angles)
    return jnp.concatenate([cos, cos], axis=-1), jnp.concatenate([-sin, sin], axis=-1)


def qkv_kernel(x_ref, wq_ref, wk_ref, wv_ref, cos_ref, sin_ref, q_ref, kv_ref):
    n_heads, head_dim = wq_ref.shape[0], wq_ref.shape[2]
    weights = jnp.concatenate([wk_ref[0], wv_ref[0]] + [wq_ref[h] for h in range(n_heads)], axis=1)
    out = jnp.dot(x_ref[...], weights, preferred_element_type=jnp.float32).astype(jnp.bfloat16)
    keys = out[:, :head_dim].astype(jnp.float32)
    keys = keys * cos_ref[...] + pltpu.roll(keys, head_dim // 2, 1) * sin_ref[...]
    kv_ref[:, :head_dim] = keys.astype(jnp.bfloat16)
    kv_ref[:, head_dim:] = out[:, head_dim:2 * head_dim]
    q_ref[...] = out[:, 2 * head_dim:]


def project_qkv(x, w_q, w_k, w_v, cos, sin):
    rows, dim = x.shape
    n_heads, _, head_dim = w_q.shape
    tile = min(rows, 256)
    row_block = lambda n: pl.BlockSpec((tile, n), lambda i: (i, 0))
    whole = lambda a: pl.BlockSpec(a.shape, lambda i: (0, 0, 0))
    return pl.pallas_call(
        qkv_kernel,
        out_shape=(jax.ShapeDtypeStruct((rows, n_heads * head_dim), jnp.bfloat16),
                   jax.ShapeDtypeStruct((rows, 2 * head_dim), jnp.bfloat16)),
        grid=(rows // tile,),
        in_specs=[row_block(dim), whole(w_q), whole(w_k), whole(w_v), row_block(head_dim), row_block(head_dim)],
        out_specs=(row_block(n_heads * head_dim), row_block(2 * head_dim)),
        compiler_params=pltpu.CompilerParams(dimension_semantics=("arbitrary",)),
        cost_estimate=pl.CostEstimate(flops=2 * rows * dim * (n_heads + 2) * head_dim, bytes_accessed=2 * (rows * dim + w_q.size), transcendentals=0),
    )(x, w_q, w_k, w_v, cos, sin)


def attn_kernel(cp, tp, chunk, groups, n_heads, scale2, cp_ref, q_ref, cos_ref, sin_ref, *refs):
    n_chunks = (len(refs) - 5)
    kv_refs = refs[:n_chunks]
    o_ref, qs, acc, m_ref, l_ref = refs[n_chunks:]
    half = tp // 2
    rows, hd = q_ref.shape[1], q_ref.shape[2] // n_heads
    t = pl.program_id(0)
    me = cp_ref[0]
    second = t >= half
    side = jnp.where(second, 1, 0)
    piece = jnp.where(second, 2 * cp - 1 - me, me)
    cosv, sinv = cos_ref[0], sin_ref[0]
    for h in range(n_heads):
        x = q_ref[0, :, h * hd:(h + 1) * hd].astype(jnp.float32)
        qs[h * rows:(h + 1) * rows, :] = (x * cosv + pltpu.roll(x, hd // 2, 1) * sinv).astype(jnp.bfloat16)
    acc[...] = jnp.zeros_like(acc)
    l_ref[...] = jnp.zeros_like(l_ref)
    m_ref[...] = jnp.full_like(m_ref, -1e30)
    total = rows * n_heads
    step = total // groups

    def update(tiles, mask):
        def score(g):
            q = qs[g * step:(g + 1) * step, :]
            out = [lax.dot_general(q, k, (((1,), (1,)), ((), ())), preferred_element_type=jnp.float32) for k, _ in tiles]
            if mask is not None:
                out[-1] = jnp.where(mask[g * step:(g + 1) * step], out[-1], -1e30)
            return out

        ahead = score(0)
        for g in range(groups):
            scores = ahead
            if g + 1 < groups:
                ahead = score(g + 1)
            sl = slice(g * step, (g + 1) * step)
            m_prev = m_ref[sl, :]
            m_cur = functools.reduce(jnp.maximum, [s[:, j * hd:(j + 1) * hd] for s in scores for j in range(s.shape[1] // hd)])
            m_new = jnp.maximum(m_prev, jnp.max(m_cur, axis=1, keepdims=True))
            alpha = jnp.exp2((m_prev - m_new) * scale2)
            l_new = l_ref[sl, :] * alpha
            a_new = acc[sl, :] * alpha
            for s, (_, v) in zip(scores, tiles):
                p = jnp.exp2((s - m_new[:, :1]) * scale2)
                for j in range(p.shape[1] // hd):
                    l_new = l_new + p[:, j * hd:(j + 1) * hd]
                a_new = a_new + jnp.dot(p.astype(jnp.bfloat16), v, preferred_element_type=jnp.float32)
            m_ref[sl, :] = m_new
            l_ref[sl, :] = l_new
            acc[sl, :] = a_new

    def load(i, j, lo, n):
        ref = kv_refs[i]
        if i < n_chunks - 1:
            j = lax.rem(me - j + cp, cp)
        k = ref[j, pl.ds(lo, n), :, :hd].reshape(n * rows, hd)
        v = ref[j, pl.ds(lo, n), :, hd:].reshape(n * rows, hd)
        return k, v

    def pair(parts):
        return (jnp.concatenate([p[0] for p in parts], axis=0), jnp.concatenate([p[1] for p in parts], axis=0))

    def full(p, carry):
        late = p >= cp
        j = jnp.where(late, 2 * cp - 1 - p, p)
        lo = jnp.where(late, half, 0)
        update([pair([load(i, j, lo, half) for i in range(n_chunks)])], None)
        return carry

    lax.fori_loop(0, piece, full, 0)
    lo = side * half

    def inner(tt, carry):
        update([pair([load(i, me, lo + tt, 1) for i in range(n_chunks)])], None)
        return carry

    lax.fori_loop(0, t - lo, inner, 0)
    n_keys = (chunk + 1) * rows
    qi = lax.broadcasted_iota(jnp.int32, (total, n_keys), 0) % rows + chunk * rows
    ki = lax.broadcasted_iota(jnp.int32, (total, n_keys), 1)
    update([pair([load(i, me, t, 1) for i in range(chunk + 1)])], qi >= ki)
    inv = 1.0 / jnp.sum(l_ref[...], axis=1, keepdims=True)
    for h in range(n_heads):
        sl = slice(h * rows, (h + 1) * rows)
        o_ref[0, :, h * hd:(h + 1) * hd] = (acc[sl, :] * inv[sl]).astype(o_ref.dtype)


def attention(q, cos, sin, kvs, me, cp, tp, chunk, n_heads, groups=5):
    _, rows, width = q.shape
    hd = width // n_heads
    scale2 = hd ** -0.5 * LOG2_E
    row_block = lambda n: pl.BlockSpec((1, rows, n), lambda t, s: (t, 0, 0))
    whole = pl.BlockSpec(kvs[0].shape, lambda t, s: (0, 0, 0, 0))
    return pl.pallas_call(
        functools.partial(attn_kernel, cp, tp, chunk, groups, n_heads, scale2),
        out_shape=jax.ShapeDtypeStruct(q.shape, jnp.bfloat16),
        grid_spec=pltpu.PrefetchScalarGridSpec(
            num_scalar_prefetch=1, grid=(tp,),
            in_specs=[row_block(width), row_block(hd), row_block(hd)] + [whole] * len(kvs),
            out_specs=row_block(width),
            scratch_shapes=[pltpu.VMEM((rows * n_heads, hd), jnp.bfloat16)] + [pltpu.VMEM((rows * n_heads, hd), jnp.float32)] * 3),
        compiler_params=pltpu.CompilerParams(dimension_semantics=("arbitrary",)),
        cost_estimate=pl.CostEstimate(flops=2 * 2 * rows * tp * n_heads * hd * rows * tp * 2, bytes_accessed=16 * 2 ** 20, transcendentals=0),
    )(me, q, cos, sin, *kvs)


def mlp_kernel(n_up, wide, x_ref, gate_ref, up_ref, down_ref, out_ref, hidden):
    i = pl.program_id(0)

    @pl.when(i < n_up)
    def _():
        weights = jnp.concatenate([gate_ref[...], up_ref[...]], axis=1)
        both = jnp.dot(x_ref[...], weights, preferred_element_type=jnp.float32)
        hidden[i] = (jax.nn.silu(both[:, :wide]) * both[:, wide:]).astype(jnp.bfloat16)

    @pl.when(i >= n_up)
    def _():
        h = jnp.concatenate([hidden[j] for j in range(n_up)], axis=1)
        out_ref[...] = jnp.dot(h, down_ref[...], preferred_element_type=jnp.float32).astype(jnp.bfloat16)


def mlp(x, w_gate, w_up, w_down, wide=384, cols=512):
    rows, dim = x.shape
    ffn = w_gate.shape[1]
    n_up, n_down = ffn // wide, dim // cols
    return pl.pallas_call(
        functools.partial(mlp_kernel, n_up, wide),
        out_shape=jax.ShapeDtypeStruct((rows, dim), jnp.bfloat16),
        grid=(n_up + n_down,),
        in_specs=[pl.BlockSpec((rows, dim), lambda i: (0, 0), pipeline_mode=pl.Buffered(1)),
                  pl.BlockSpec((dim, wide), lambda i: (0, jnp.minimum(i, n_up - 1))),
                  pl.BlockSpec((dim, wide), lambda i: (0, jnp.minimum(i, n_up - 1))),
                  pl.BlockSpec((ffn, cols), lambda i: (0, jnp.maximum(i - n_up, 0)))],
        out_specs=pl.BlockSpec((rows, cols), lambda i: (0, jnp.maximum(i - n_up, 0))),
        scratch_shapes=[pltpu.VMEM((n_up, rows, wide), jnp.bfloat16)],
        compiler_params=pltpu.CompilerParams(dimension_semantics=("arbitrary",)),
        cost_estimate=pl.CostEstimate(flops=6 * rows * dim * ffn, bytes_accessed=6 * dim * ffn, transcendentals=0),
    )(x, w_gate, w_up, w_down)


def up_kernel(wide, x_ref, gate_ref, up_ref, hidden_ref):
    weights = jnp.concatenate([gate_ref[...], up_ref[...]], axis=1)
    both = jnp.dot(x_ref[...], weights, preferred_element_type=jnp.float32)
    hidden_ref[...] = (jax.nn.silu(both[:, :wide]) * both[:, wide:]).astype(jnp.bfloat16)


def mlp_up(x, w_gate, w_up, wide=384):
    rows, dim = x.shape
    ffn = w_gate.shape[1]
    return pl.pallas_call(
        functools.partial(up_kernel, wide),
        out_shape=jax.ShapeDtypeStruct((rows, ffn), jnp.bfloat16),
        grid=(ffn // wide,),
        in_specs=[pl.BlockSpec((rows, dim), lambda i: (0, 0), pipeline_mode=pl.Buffered(1)),
                  pl.BlockSpec((dim, wide), lambda i: (0, i)), pl.BlockSpec((dim, wide), lambda i: (0, i))],
        out_specs=pl.BlockSpec((rows, wide), lambda i: (0, i)),
        compiler_params=pltpu.CompilerParams(dimension_semantics=("arbitrary",)),
        cost_estimate=pl.CostEstimate(flops=4 * rows * dim * ffn, bytes_accessed=4 * dim * ffn, transcendentals=0),
    )(x, w_gate, w_up)


def down_kernel(h_ref, down_ref, out_ref):
    out_ref[...] = jnp.dot(h_ref[...], down_ref[...], preferred_element_type=jnp.float32).astype(jnp.bfloat16)


def mlp_down(hidden, w_down, cols=512):
    rows, ffn = hidden.shape
    dim = w_down.shape[1]
    return pl.pallas_call(
        down_kernel,
        out_shape=jax.ShapeDtypeStruct((rows, dim), jnp.bfloat16),
        grid=(dim // cols,),
        in_specs=[pl.BlockSpec((rows, ffn), lambda i: (0, 0), pipeline_mode=pl.Buffered(1)),
                  pl.BlockSpec((ffn, cols), lambda i: (0, i))],
        out_specs=pl.BlockSpec((rows, cols), lambda i: (0, i)),
        compiler_params=pltpu.CompilerParams(dimension_semantics=("arbitrary",)),
        cost_estimate=pl.CostEstimate(flops=2 * rows * dim * ffn, bytes_accessed=2 * dim * ffn, transcendentals=0),
    )(hidden, w_down)


def solution(mesh):
    cp_size, tp_size = mesh.shape['cp'], mesh.shape['tp']
    row_spec = P('dp', ('cp', 'tp'), None)
    head_cols = P(None, 'tp', None)

    def local_layer(x, g_attn, w_q, w_k, w_v, w_o, g_mlp, w_gate, w_up, w_down):
        x_rows = x[0]
        n_own, dim = x_rows.shape
        n_heads, head_dim = w_q.shape[1], w_q.shape[2]
        cp_index = lax.axis_index('cp')
        seq_local = n_own * tp_size
        piece_len = seq_local // 2
        rows = n_own // N_CHUNKS
        wq_t, wk_t, wv_t = (jnp.transpose(w, (1, 0, 2)) for w in (w_q, w_k, w_v))
        w_o_flat = w_o.reshape(n_heads * head_dim, dim)

        within = jnp.arange(seq_local, dtype=jnp.int32)
        positions = jnp.where(within < piece_len, cp_index * piece_len + within,
                              (2 * cp_size - 1 - cp_index) * piece_len + within - piece_len)
        cos, sin = rope_tables(positions, head_dim)
        by_owner = lambda a: a.reshape(tp_size, N_CHUNKS, rows, a.shape[-1])
        cos, sin = by_owner(cos), by_owner(sin)

        normed = rms_norm(x_rows, g_attn)
        gathered = [lax.all_gather(normed[c * rows:(c + 1) * rows], 'tp', axis=0, tiled=True) for c in range(N_CHUNKS)]
        qs, kvs = [], []
        for c in range(N_CHUNKS):
            flat = lambda a: a[:, c].reshape(tp_size * rows, head_dim)
            q, kv = project_qkv(gathered[c], wq_t, wk_t, wv_t, flat(cos), flat(sin))
            qs.append(q.reshape(tp_size, rows, n_heads * head_dim))
            kv = kv.reshape(tp_size, rows, 2 * head_dim)
            if c == N_CHUNKS - 1:
                kvs.append(lax.all_gather(kv, 'cp', axis=0, tiled=False))
            else:
                shifted = [lax.ppermute(kv, 'cp', [(i, (i + d) % cp_size) for i in range(cp_size)]) for d in range(1, cp_size)]
                kvs.append(jnp.stack([kv] + shifted))
                gathered[c + 1], kvs[c] = lax.optimization_barrier((gathered[c + 1], kvs[c]))

        me = cp_index.astype(jnp.int32).reshape(1)
        sub = n_own // MLP_CHUNKS
        per = rows // sub
        mixed = [attention(qs[c], cos[:, c], sin[:, c], kvs, me, cp_size, tp_size, c, n_heads, 2) for c in range(N_CHUNKS)]

        def attn_out(mixed_c):
            return jnp.dot(mixed_c.reshape(tp_size * rows, n_heads * head_dim), w_o_flat,
                           preferred_element_type=jnp.float32).astype(jnp.bfloat16)

        def mlp_in(c, attn_rows):
            own = attn_rows[(c % per) * sub:(c % per + 1) * sub]
            resid = (x_rows[c * sub:(c + 1) * sub].astype(jnp.float32) + own.astype(jnp.float32)).astype(jnp.bfloat16)
            return resid, rms_norm(resid, g_mlp)

        scatter = lambda a: lax.psum_scatter(a, 'tp', scatter_dimension=0, tiled=True)
        gather = lambda a: lax.all_gather(a, 'tp', axis=0, tiled=True)
        whole_mlp = lambda a: mlp(a, w_gate, w_up, w_down)

        attn_0 = scatter(attn_out(mixed[0]))
        first = [mlp_in(c, attn_0) for c in range(per)]
        mixed_1, first = lax.optimization_barrier((mixed[1], first))
        arrived = [gather(r) for _, r in first]
        part_1, arrived[0] = lax.optimization_barrier((attn_out(mixed_1), arrived[0]))
        attn_1 = scatter(part_1)
        down_0, arrived[1] = lax.optimization_barrier((whole_mlp(arrived[0]), arrived[1]))
        down = [down_0]
        hidden = mlp_up(arrived[1], w_gate, w_up)
        hidden, attn_1 = lax.optimization_barrier((hidden, attn_1))
        later = [mlp_in(per + c, attn_1) for c in range(per)]
        hidden, later = lax.optimization_barrier((hidden, later))
        down.append(mlp_down(hidden, w_down))
        down += [whole_mlp(gather(r)) for _, r in later]
        resid = [r for r, _ in first + later]
        outs = [(r.astype(jnp.float32) + scatter(d).astype(jnp.float32)).astype(jnp.bfloat16) for r, d in zip(resid, down)]
        return jnp.concatenate(outs, axis=0)[None]

    return jax.shard_map(local_layer, mesh=mesh,
                         in_specs=(row_spec, P(), head_cols, head_cols, head_cols, P('tp', None, None),
                                   P(), P(None, 'tp'), P(None, 'tp'), P('tp', None)),
                         out_specs=row_spec, check_vma=False)
```
